256 devices in a mesh: slab: 2 (over z), wide: 128 (over x, y, core).
Axes of the slice: x: 8, y: 8, z: 2, core: 2. Of those that a mesh axis runs over, the one named last changes fastest.
The devices are a block of a 8x8x16 slice.
Arguments:
- slc: bfloat16 [128, 4096, 2, 512], P('wide', 'slab'), parts along dimension 1, may hold values from -10 to 10
- offsets: bfloat16 [128, 4096], P('wide', 'slab'), parts along dimension 1, may hold values from -0.5 to 0.5
- row_start: int32 [128], replicated, may hold values from 0 to 127
- row_stop: int32 [128], replicated, may hold values from 385 to 512
- pairs: int32 [512, 2], replicated, may hold values from 0 to 127, as said below
Outputs:
- coherence: bfloat16 [8192, 2, 128, 128], P(('slab', 'wide')), parts along dimension 0
- flattened: float32 [8192, 2, 512], P(('slab', 'wide')), parts along dimension 0
- ramps: float32 [1024, 2, 3], P(('slab', 'wide')), parts along dimension 0
The draws below stay inside these ranges and needn't reach their ends.
There are 2 independent parts, one for each index of `slab`. The reference program is written for one: setup_inputs(seed, part) draws one part's arguments, and reference() takes and returns one part's arrays. A program takes and returns all parts, laid end to end along the dimension named above; an argument that names none is the same for every part. Nothing has to cross between parts.
Inputs may be any that keep to these rules, and one draw needn't show every extreme that they name: `pairs`: each row names two different dates.
All inputs are finite; a program needn't handle non-finite values.
Results may differ from the reference program's by a relative error of at most 0.0098.
Values may be sent and summed in bfloat16 or wider, within the bound.
No kernel may reach another device: no remote copies, remote signals or barrier semaphores. Data moves between devices by JAX's collectives and lax.ppermute only.
A program may use at most 128 MiB of HBM per device.

```python
import math
import jax
import jax.numpy as jnp
from jax import lax

DATES = 128
AZ = 512
LOOK_AZ = 16
LOOK_RG = 16
COLS = 2048
PAIRS = 512
CELLS = 4096


def draw_slc(key, part):
    base_key = jax.random.fold_in(key, 101)
    field_key, date_key = jax.random.split(base_key)
    speckle = jax.random.normal(field_key, (2, COLS, AZ + 2), jnp.float32)
    scatter = (speckle[:, :, :-2] + speckle[:, :, 1:-1] + speckle[:, :, 2:]) * 0.58
    across = jnp.arange(COLS, dtype=jnp.float32) / COLS - 0.5
    along = jnp.arange(AZ, dtype=jnp.float32) / AZ - 0.5
    date_keys = jax.random.split(date_key, DATES)

    def one_date(subkey):
        slope_key, phase_key, noise_key = jax.random.split(subkey, 3)
        slopes = jax.random.uniform(slope_key, (3,), jnp.float32, -4.0, 4.0)
        rotation = slopes[0] + 2.0 * math.pi * (slopes[1] * across[:, None] + slopes[2] * along[None, :])
        rotation = rotation + 0.4 * jax.random.normal(phase_key, (COLS, AZ), jnp.float32)
        noise = 0.35 * jax.random.normal(noise_key, (2, COLS, AZ), jnp.float32)
        cos_rot, sin_rot = (jnp.cos(rotation), jnp.sin(rotation))
        real_part = scatter[0] * cos_rot - scatter[1] * sin_rot + noise[0]
        imag_part = scatter[0] * sin_rot + scatter[1] * cos_rot + noise[1]
        return jnp.clip(jnp.stack([real_part, imag_part], 1), -10.0, 10.0)
    return lax.map(one_date, date_keys).astype(jnp.bfloat16)


def draw_pairs(key, part):
    first_key, second_key = jax.random.split(jax.random.fold_in(key, 23))
    first_date = jax.random.randint(first_key, (PAIRS,), 0, DATES, jnp.int32)
    gap_dates = jax.random.randint(second_key, (PAIRS,), 1, DATES, jnp.int32)
    second_date = (first_date + gap_dates) % DATES
    return jnp.stack([first_date, second_date], 1).astype(jnp.int32)


def with_ends(drawn, stream_key, least, largest):
    index_at = [jax.random.randint(jax.random.fold_in(stream_key, axis), (), 0, length) for axis, length in enumerate(drawn.shape)]
    widest = drawn.shape.index(max(drawn.shape))
    beside = index_at[:widest] + [(index_at[widest] + 1) % drawn.shape[widest]] + index_at[widest + 1:]
    return drawn.at[tuple(index_at)].set(least).at[tuple(beside)].set(largest)


def steps_of(stream_key, shape, shards, smallest, top_value):
    def one(dim, shards_of):
        steps = jax.random.uniform(jax.random.fold_in(jax.random.fold_in(stream_key, 6), dim), (shards_of,), jnp.float32, smallest / len(shards), top_value / len(shards))
        return jnp.repeat(jnp.exp(steps), shape[dim] // shards_of).reshape((-1,) + (1,) * (len(shape) - dim - 1))

    level = one(*shards[0])
    for cut in shards[1:]:
        level = level * one(*cut)
    return level


def setup_inputs(seed: int = 0, part: int = 0) -> dict:
    splits = jax.random.split(jax.random.key(seed), 6)
    own_keys = jax.random.split(jax.random.fold_in(splits[5], part), 6)
    return {
        "slc": draw_slc(jax.random.fold_in(jax.random.fold_in(splits[5], part), 71), part),
        "offsets": jnp.clip(jax.random.uniform(own_keys[1], (DATES, COLS), jnp.float32, -0.5, 0.5) * steps_of(own_keys[1], (DATES, COLS), ((0, 128),), -0.4, 0.0), -0.5, 0.5).astype(jnp.bfloat16),
        "row_start": with_ends(jax.random.randint(splits[2], (DATES,), 0, AZ // 4), jax.random.fold_in(splits[2], 1), 0, (AZ // 4) - 1).astype(jnp.int32),
        "row_stop": with_ends(jax.random.randint(splits[3], (DATES,), AZ - AZ // 4 + 1, AZ + 1), jax.random.fold_in(splits[3], 1), AZ - AZ // 4 + 1, AZ).astype(jnp.int32),
        "pairs": draw_pairs(jax.random.fold_in(splits[5], 71), part),
    }


damping = 1.0

def tables(size):
    ordinal = jnp.arange(size, dtype=jnp.int32)
    product = ordinal[:, None] * ordinal[None, :] % size
    angles = product.astype(jnp.float32) * (2.0 * math.pi / size)
    cosine = jnp.cos(angles).astype(jnp.bfloat16)
    sine_table = jnp.sin(angles).astype(jnp.bfloat16)
    forward = jnp.concatenate([jnp.concatenate([cosine, -sine_table], 1), jnp.concatenate([sine_table, cosine], 1)], 0)
    inverse = jnp.concatenate([jnp.concatenate([cosine, sine_table], 1), jnp.concatenate([-sine_table, cosine], 1)], 0)
    return (forward, inverse)

def resample(samples, shifts, start_rows, stop_rows, forward, inverse):
    date_count, columns_here = (samples.shape[0], samples.shape[1])
    row_index = jnp.arange(AZ, dtype=jnp.int32)
    valid_rows = ((row_index[None, :] >= start_rows[:, None]) & (row_index[None, :] < stop_rows[:, None])).astype(samples.dtype)
    masked = samples * valid_rows[:, None, None, :]
    stacked = masked.reshape(date_count * columns_here, 2 * AZ)
    spectrum = jnp.dot(stacked, forward, preferred_element_type=jnp.float32).astype(jnp.bfloat16)
    spectrum = lax.optimization_barrier(spectrum).astype(jnp.float32)
    frequency = jnp.where(row_index < AZ // 2, row_index, row_index - AZ).astype(jnp.float32)
    rotation = -2.0 * math.pi / AZ * frequency[None, :] * shifts.astype(jnp.float32).reshape(date_count * columns_here, 1)
    cos_rot, sin_rot = (jnp.cos(rotation), jnp.sin(rotation))
    spec_real, spec_imag = (spectrum[:, :AZ], spectrum[:, AZ:])
    turned = jnp.concatenate([spec_real * cos_rot - spec_imag * sin_rot, spec_real * sin_rot + spec_imag * cos_rot], 1).astype(jnp.bfloat16)
    restored = jnp.dot(turned, inverse, preferred_element_type=jnp.float32) * (1.0 / AZ)
    return restored.astype(jnp.bfloat16).reshape(date_count, columns_here, 2, AZ)

def coherence_cells(columns):
    date_count, columns_here = (columns.shape[0], columns.shape[1])
    range_cells = columns_here // LOOK_RG
    line_cells = AZ // LOOK_AZ
    pixels = columns.reshape(date_count, range_cells, LOOK_RG, 2, line_cells, LOOK_AZ).transpose(1, 4, 3, 0, 2, 5)
    pixels = pixels.reshape(range_cells * line_cells, 2, date_count, LOOK_RG * LOOK_AZ)
    real_part, imag_part = (pixels[:, 0], pixels[:, 1])
    stacked = jnp.concatenate([real_part, imag_part], -1)
    partner = jnp.concatenate([stacked, jnp.concatenate([-imag_part, real_part], -1)], 1)
    covariance = jnp.einsum('gdp,gep->gde', stacked.astype(jnp.float32), partner.astype(jnp.float32))
    intensity = jnp.diagonal(covariance[:, :, :date_count], axis1=1, axis2=2) + damping
    normalizer = lax.rsqrt(intensity[:, :, None] * intensity[:, None, :])
    normalizer = jnp.concatenate([normalizer, normalizer], -1)
    coherent = covariance * normalizer
    return coherent.reshape(-1, date_count, 2, date_count).transpose(0, 2, 1, 3)

def select_pairs(coherent, pairs):
    first_date, second_date = (pairs[:, 0], pairs[:, 1])
    chosen_rows = jnp.take(coherent, first_date, axis=2)
    chooser = (jnp.arange(coherent.shape[3], dtype=jnp.int32)[None, :] == second_date[:, None]).astype(jnp.float32)
    return lax.optimization_barrier(jnp.sum(chosen_rows * chooser[None, None], -1))

def cell_design(cell_index, range_cells):
    line_cells = AZ // LOOK_AZ
    line_pos = (cell_index % line_cells).astype(jnp.float32)
    range_pos = (cell_index // line_cells).astype(jnp.float32)
    across = (line_pos + 0.5) / line_cells - 0.5
    along = (range_pos + 0.5) / range_cells - 0.5
    return jnp.stack([jnp.ones_like(across), across, along], 1)

def normal_terms(interferograms, design):
    weights = 0.1 + interferograms[:, 0] ** 2 + interferograms[:, 1] ** 2
    products = jnp.stack([design[:, 0] * design[:, 0], design[:, 0] * design[:, 1], design[:, 0] * design[:, 2], design[:, 1] * design[:, 1], design[:, 1] * design[:, 2], design[:, 2] * design[:, 2]], 1)
    normal = lax.optimization_barrier(jnp.sum(products[:, :, None] * weights[:, None, :], 0)).T
    target = lax.optimization_barrier(jnp.sum((interferograms * weights[:, None, :])[..., None] * design[:, None, None, :], 0))
    return (normal, target.transpose(1, 0, 2))

def solve_three(normal, target):
    top_left, top_mid, top_right = (normal[:, 0], normal[:, 1], normal[:, 2])
    mid_mid, mid_right, low_right = (normal[:, 3], normal[:, 4], normal[:, 5])
    adjugate_00 = mid_mid * low_right - mid_right * mid_right
    adjugate_01 = top_right * mid_right - top_mid * low_right
    adjugate_02 = top_mid * mid_right - top_right * mid_mid
    adjugate_11 = top_left * low_right - top_right * top_right
    adjugate_12 = top_mid * top_right - top_left * mid_right
    adjugate_22 = top_left * mid_mid - top_mid * top_mid
    determinant = top_left * adjugate_00 + top_mid * adjugate_01 + top_right * adjugate_02
    first_rhs, second_rhs, third_rhs = (target[..., 0], target[..., 1], target[..., 2])
    first_out = adjugate_00[:, None] * first_rhs + adjugate_01[:, None] * second_rhs + adjugate_02[:, None] * third_rhs
    second_out = adjugate_01[:, None] * first_rhs + adjugate_11[:, None] * second_rhs + adjugate_12[:, None] * third_rhs
    third_out = adjugate_02[:, None] * first_rhs + adjugate_12[:, None] * second_rhs + adjugate_22[:, None] * third_rhs
    return jnp.stack([first_out, second_out, third_out], -1) / determinant[:, None, None]

def ramp_values(coefficients, design):
    return lax.optimization_barrier(jnp.sum(design[:, None, None, :] * coefficients.transpose(1, 0, 2)[None], -1))

def reference(slc, offsets, row_start, row_stop, pairs):
    forward, inverse = tables(AZ)

    def one_date(element):
        samples, shifts, start_rows, stop_rows = element
        return resample(samples[None], shifts[None], start_rows[None], stop_rows[None], forward, inverse)[0]
    resampled = lax.map(one_date, (slc, offsets, row_start, row_stop))
    range_cells = COLS // LOOK_RG

    def one_range(position):
        columns = lax.dynamic_slice_in_dim(resampled, position * LOOK_RG, LOOK_RG, 1)
        return coherence_cells(columns)
    coherent = lax.map(one_range, jnp.arange(range_cells, dtype=jnp.int32))
    coherent = coherent.reshape(CELLS, 2, DATES, DATES)
    interferograms = select_pairs(coherent, pairs)
    design = cell_design(jnp.arange(CELLS, dtype=jnp.int32), range_cells)
    normal, target = normal_terms(interferograms, design)
    coefficients = solve_three(normal, target)
    flattened = interferograms - ramp_values(coefficients, design)
    return (coherent.astype(jnp.bfloat16), flattened, coefficients)
```

```python
import math

import jax
import jax.numpy as jnp
from jax import lax
from jax.experimental import pallas as pl
from jax.experimental.pallas import tpu as pltpu
from jax.sharding import Mesh
from jax.sharding import PartitionSpec as P

AZ = 512
LOOK_AZ = 16
LOOK_RG = 16
LINE_CELLS = AZ // LOOK_AZ
WIDE = ("wide_0", "wide_1", "wide_2")
SLAB_WIDE = ("slab", "wide_0", "wide_1", "wide_2")
DAMPING = 1.0
COLS_STEP = 4
CELLS_STEP = 4
ROT_ROWS = 16


def spectral_table():
    ordinal = jnp.arange(AZ, dtype=jnp.int32)
    product = ordinal[:, None] * ordinal[None, :] % AZ
    angles = product.astype(jnp.float32) * (2.0 * math.pi / AZ)
    cosine = jnp.cos(angles).astype(jnp.bfloat16)
    sine = jnp.sin(angles).astype(jnp.bfloat16)
    return jnp.concatenate(
        [jnp.concatenate([cosine, -sine], 1), jnp.concatenate([sine, cosine], 1)], 0
    )


def exchange_small(rows):
    count = rows.shape[0]
    index = jnp.arange(count, dtype=jnp.int32)[:, None]
    stride = 1
    for axis in reversed(WIDE):
        size = lax.axis_size(axis)
        own = lax.axis_index(axis)
        step = 1
        while step < size:
            bit = (own // step) % 2
            got = lax.ppermute(rows, axis, [(i, i ^ step) for i in range(size)])
            got = jnp.where(bit == 0, jnp.roll(got, stride, 0), jnp.roll(got, -stride, 0))
            rows = jnp.where((index // stride) % 2 == bit, rows, got)
            stride *= 2
            step *= 2
    return rows


def rotated(spectrum, shift, frequency):
    z = frequency * shift
    zz = z * z
    sin_rot = z * (
        1.0
        + zz
        * (
            -1.0 / 6
            + zz * (1.0 / 120 + zz * (-1.0 / 5040 + zz * (1.0 / 362880 + zz * (-1.0 / 39916800))))
        )
    )
    cos_rot = 1.0 + zz * (
        -0.5
        + zz
        * (
            1.0 / 24
            + zz
            * (
                -1.0 / 720
                + zz * (1.0 / 40320 + zz * (-1.0 / 3628800 + zz * (1.0 / 479001600)))
            )
        )
    )
    real, imag = spectrum[:, :AZ], spectrum[:, AZ:]
    return jnp.concatenate(
        [real * cos_rot - imag * sin_rot, real * sin_rot + imag * cos_rot], 1
    )


def cells_kernel(
    x_ref, valid_ref, shift_ref, table_ref, second_ref, first_ref, coh_ref, ifg_ref, sums_ref,
    spec_ref, turned_ref, pix_ref, int_ref,
):
    step = pl.program_id(0)
    dates = valid_ref.shape[0]
    range_steps = LOOK_RG // COLS_STEP

    @pl.when(step < range_steps)
    def _resample():
        valid = valid_ref[...]
        parts = []
        for part in range(2):
            parts.append(
                jnp.concatenate([x_ref[c, part] * valid for c in range(COLS_STEP)], 0)
            )
        stacked = jnp.concatenate(parts, 1)
        spec_ref[...] = jnp.dot(
            stacked, table_ref[...], preferred_element_type=jnp.float32
        ).astype(jnp.bfloat16)
        bins = lax.broadcasted_iota(jnp.int32, (1, AZ), 1)
        frequency = jnp.where(bins < AZ // 2, bins, bins - AZ).astype(jnp.float32)
        frequency = frequency * (-2.0 * math.pi / AZ)

        def turn(i, _):
            rows = pl.ds(pl.multiple_of(i * ROT_ROWS, ROT_ROWS), ROT_ROWS)
            turned_ref[rows, :] = rotated(
                spec_ref[rows, :].astype(jnp.float32), shift_ref[rows, :], frequency
            ).astype(jnp.bfloat16)
            return _

        lax.fori_loop(0, COLS_STEP * dates // ROT_ROWS, turn, None)
        restored = lax.dot_general(
            table_ref[...], turned_ref[...], (((1,), (1,)), ((), ())),
            preferred_element_type=jnp.float32,
        )
        restored = (restored * (1.0 / AZ)).astype(jnp.bfloat16)
        for c in range(COLS_STEP):
            pix_ref[:, :, step * COLS_STEP + c] = restored[
                :, c * dates : (c + 1) * dates
            ].reshape(2, LINE_CELLS, LOOK_AZ, dates)

    @pl.when(step >= range_steps)
    def _covariance():
        diagonal = lax.broadcasted_iota(jnp.int32, (dates, dates), 0) == lax.broadcasted_iota(
            jnp.int32, (dates, dates), 1
        )
        base = (step - range_steps) * CELLS_STEP

        def cell_of(k, _):
            cell = base + k
            real = pix_ref[0, cell].reshape(LOOK_RG * LOOK_AZ, dates)
            imag = pix_ref[1, cell].reshape(LOOK_RG * LOOK_AZ, dates)
            pixels = jnp.concatenate([real, imag], 0)
            partner = jnp.concatenate([pixels, jnp.concatenate([-imag, real], 0)], 1)
            cov = lax.dot_general(
                pixels, partner, (((0,), (0,)), ((), ())), preferred_element_type=jnp.float32
            )
            on_diagonal = jnp.where(diagonal, cov[:, :dates], 0.0)
            scale_rows = lax.rsqrt(jnp.sum(on_diagonal, 1, keepdims=True) + DAMPING)
            scale_cols = lax.rsqrt(jnp.sum(on_diagonal, 0, keepdims=True) + DAMPING)
            scale = scale_rows * scale_cols
            gamma = jnp.concatenate([cov[:, :dates] * scale, cov[:, dates:] * scale], 0)
            high = gamma.astype(jnp.bfloat16)
            coh_ref[k] = high.reshape(2, dates, dates)
            low = (gamma - high.astype(jnp.float32)).astype(jnp.bfloat16)
            picked = jnp.dot(
                jnp.concatenate([high, low], 1), second_ref[...], preferred_element_type=jnp.float32
            )
            first = first_ref[...]
            int_ref[cell, 0:1, :] = jnp.sum(picked[:dates] * first, 0, keepdims=True)
            int_ref[cell, 1:2, :] = jnp.sum(picked[dates:] * first, 0, keepdims=True)
            return _

        lax.fori_loop(0, CELLS_STEP, cell_of, None)

    @pl.when(step == pl.num_programs(0) - 1)
    def _sums():
        ifg = int_ref[...]
        ifg_ref[...] = ifg
        real, imag = ifg[:, 0, :], ifg[:, 1, :]
        weight = 0.1 + real * real + imag * imag
        across = (lax.broadcasted_iota(jnp.int32, (LINE_CELLS, 1), 0).astype(jnp.float32) + 0.5) / LINE_CELLS - 0.5
        tilted = weight * across
        terms = (weight, tilted, tilted * across, weight * real, tilted * real, weight * imag, tilted * imag)
        for k, term in enumerate(terms):
            sums_ref[k : k + 1, :] = jnp.sum(term, 0, keepdims=True)
        sums_ref[len(terms) :, :] = jnp.zeros_like(sums_ref[len(terms) :, :])


def cells_call(x, valid, shifts, table, second, first):
    dates = valid.shape[0]
    pairs = first.shape[1]
    range_steps = LOOK_RG // COLS_STEP
    steps = range_steps + LINE_CELLS // CELLS_STEP
    last = range_steps - 1
    whole = lambda *shape: pl.BlockSpec(shape, lambda s: (0,) * len(shape))
    rows = COLS_STEP * dates
    return pl.pallas_call(
        cells_kernel,
        grid=(steps,),
        in_specs=[
            pl.BlockSpec((COLS_STEP, 2, dates, AZ), lambda s: (jnp.minimum(s, last), 0, 0, 0)),
            whole(dates, AZ),
            pl.BlockSpec((rows, 1), lambda s: (jnp.minimum(s, last), 0)),
            whole(2 * AZ, 2 * AZ),
            whole(2 * dates, pairs),
            whole(dates, pairs),
        ],
        out_specs=[
            pl.BlockSpec(
                (CELLS_STEP, 2, dates, dates), lambda s: (jnp.maximum(s - range_steps, 0), 0, 0, 0)
            ),
            whole(LINE_CELLS, 2, pairs),
            whole(8, pairs),
        ],
        out_shape=[
            jax.ShapeDtypeStruct((LINE_CELLS, 2, dates, dates), jnp.bfloat16),
            jax.ShapeDtypeStruct((LINE_CELLS, 2, pairs), jnp.float32),
            jax.ShapeDtypeStruct((8, pairs), jnp.float32),
        ],
        scratch_shapes=[
            pltpu.VMEM((rows, 2 * AZ), jnp.bfloat16),
            pltpu.VMEM((rows, 2 * AZ), jnp.bfloat16),
            pltpu.VMEM((2, LINE_CELLS, LOOK_RG, LOOK_AZ, dates), jnp.bfloat16),
            pltpu.VMEM((LINE_CELLS, 2, pairs), jnp.float32),
        ],
        compiler_params=pltpu.CompilerParams(dimension_semantics=("arbitrary",)),
        name="cells",
    )(x, valid, shifts, table, second, first)


def plane_sums(gathered, first_range, range_cells):
    along = (first_range + jnp.arange(gathered.shape[0], dtype=jnp.int32)).astype(jnp.float32)
    along = ((along + 0.5) / range_cells - 0.5)[:, None]
    w0, w1, w2, r0, r1, i0, i1 = (gathered[:, k] for k in range(7))
    terms = (w0, w1, w0 * along, w2, w1 * along, w0 * along * along, r0, r1, r0 * along, i0, i1, i0 * along)
    return jnp.stack([jnp.sum(t, 0) for t in terms], 0)


def solve_three(n):
    adjugate_00 = n[3] * n[5] - n[4] * n[4]
    adjugate_01 = n[2] * n[4] - n[1] * n[5]
    adjugate_02 = n[1] * n[4] - n[2] * n[3]
    adjugate_11 = n[0] * n[5] - n[2] * n[2]
    adjugate_12 = n[1] * n[2] - n[0] * n[4]
    adjugate_22 = n[0] * n[3] - n[1] * n[1]
    determinant = n[0] * adjugate_00 + n[1] * adjugate_01 + n[2] * adjugate_02
    parts = []
    for t in (n[6:9], n[9:12]):
        parts.append(
            jnp.stack(
                [
                    adjugate_00 * t[0] + adjugate_01 * t[1] + adjugate_02 * t[2],
                    adjugate_01 * t[0] + adjugate_11 * t[1] + adjugate_12 * t[2],
                    adjugate_02 * t[0] + adjugate_12 * t[1] + adjugate_22 * t[2],
                ],
                0,
            )
            / determinant
        )
    return jnp.stack(parts, 0)


def shared_by_all(array, axes):
    size = 1
    for a in (axes if isinstance(axes, tuple) else (axes,)):
        size *= lax.axis_size(a)
    copies = jnp.broadcast_to(array[None], (size, *array.shape))
    return lax.all_to_all(copies, axes, 0, 0, tiled=True)


def local(slc, offsets, row_start, row_stop, pairs):
    devices = lax.axis_size(WIDE)
    position = lax.axis_index(WIDE)
    columns = slc.shape[1]
    dates = devices * slc.shape[0]
    received = lax.all_to_all(
        slc.reshape(devices, columns // devices, 2, AZ), WIDE, 0, 0, tiled=True
    )
    x = received.transpose(1, 2, 0, 3)
    shifts = exchange_small(offsets.reshape(devices, columns // devices))
    shifts = shifts.astype(jnp.float32).T.reshape(-1, 1)
    lines = jnp.arange(AZ, dtype=jnp.int32)[None, :]
    valid = ((lines >= row_start[:, None]) & (lines < row_stop[:, None])).astype(jnp.bfloat16)
    date = jnp.arange(dates, dtype=jnp.int32)[:, None]
    first = (date == pairs[:, 0][None, :]).astype(jnp.float32)
    second = (date == pairs[:, 1][None, :]).astype(jnp.bfloat16)
    second = jnp.concatenate([second, second], 0)
    coherence, ifg, sums = cells_call(x, valid, shifts, spectral_table(), second, first)

    range_cells = columns // LOOK_RG
    near = lax.axis_size(("wide_1", "wide_2"))
    gathered = shared_by_all(sums, ("wide_1", "wide_2"))
    partial = plane_sums(gathered, lax.axis_index("wide_0") * near, range_cells)
    total = jnp.sum(shared_by_all(partial, "wide_0"), 0)
    ramps = solve_three(total)
    share = pairs.shape[0] // devices
    own = lax.dynamic_slice_in_dim(ramps, position * share, share, 2).transpose(2, 0, 1)
    across = (jnp.arange(LINE_CELLS, dtype=jnp.int32).astype(jnp.float32) + 0.5) / LINE_CELLS - 0.5
    along = (position.astype(jnp.float32) + 0.5) / range_cells - 0.5
    plane = ramps[:, 0] + across[:, None, None] * ramps[:, 1] + along * ramps[:, 2]
    return coherence, ifg - plane, own


def solution(mesh):
    torus = Mesh(
        mesh.devices.reshape(mesh.shape["slab"], 8, 8, 2), ("slab", "wide_0", "wide_1", "wide_2")
    )
    in_specs = (P(WIDE, "slab", None, None), P(WIDE, "slab"), P(), P(), P())
    out_specs = (P(SLAB_WIDE, None, None, None), P(SLAB_WIDE, None, None), P(SLAB_WIDE, None, None))
    return jax.shard_map(local, mesh=torus, in_specs=in_specs, out_specs=out_specs, check_vma=False)
```

```python
import math

import jax
import jax.numpy as jnp
from jax import lax
from jax.experimental import pallas as pl
from jax.experimental.pallas import tpu as pltpu
from jax.sharding import Mesh
from jax.sharding import PartitionSpec as P

AZ = 512
LOOK_AZ = 16
LOOK_RG = 16
LINE_CELLS = AZ // LOOK_AZ
WIDE = ("wide_0", "wide_1", "wide_2")
SLAB_WIDE = ("slab", "wide_0", "wide_1", "wide_2")
DAMPING = 1.0
DATES_STEP = 32
COLS_STEP = 8
CELLS_STEP = 8
ROT_ROWS = 16
LANES = 128
BLOCKS = AZ // LANES
COL_ROWS = 2 * BLOCKS
PACK_STEPS = 4


def spectral_table():
    ordinal = jnp.arange(AZ, dtype=jnp.int32)
    product = ordinal[:, None] * ordinal[None, :] % AZ
    angles = product.astype(jnp.float32) * (2.0 * math.pi / AZ)
    cosine = jnp.cos(angles).astype(jnp.bfloat16)
    sine = jnp.sin(angles).astype(jnp.bfloat16)
    return jnp.concatenate(
        [jnp.concatenate([cosine, -sine], 1), jnp.concatenate([sine, cosine], 1)], 0
    )


def pack_kernel(samples_ref, extra_ref, out_ref, buffer, extra_buffer, in_sem, out_sem):
    share = samples_ref.shape[0] // PACK_STEPS
    width = samples_ref.shape[1]
    rows = [pl.ds(i * share, share) for i in range(PACK_STEPS)]
    extra_in = pltpu.make_async_copy(extra_ref, extra_buffer, in_sem.at[PACK_STEPS])
    extra_out = pltpu.make_async_copy(
        extra_buffer, out_ref.at[:, pl.ds(width, 1)], out_sem.at[PACK_STEPS]
    )
    ins = [
        pltpu.make_async_copy(samples_ref.at[rows[i]], buffer.at[rows[i]], in_sem.at[i])
        for i in range(PACK_STEPS)
    ]
    outs = [
        pltpu.make_async_copy(
            buffer.at[rows[i]], out_ref.at[rows[i], pl.ds(0, width)], out_sem.at[i]
        )
        for i in range(PACK_STEPS)
    ]
    extra_in.start()
    for copy in ins:
        copy.start()
    extra_in.wait()
    extra_out.start()
    for copy_in, copy_out in zip(ins, outs):
        copy_in.wait()
        copy_out.start()
    extra_out.wait()
    for copy in outs:
        copy.wait()


def packed(samples, extra):
    devices, width = samples.shape[:2]
    return pl.pallas_call(
        pack_kernel,
        in_specs=[pl.BlockSpec(memory_space=pl.ANY)] * 2,
        out_specs=pl.BlockSpec(memory_space=pl.ANY),
        out_shape=jax.ShapeDtypeStruct((devices, width + 1, 2, LANES), samples.dtype),
        scratch_shapes=[
            pltpu.VMEM(samples.shape, samples.dtype),
            pltpu.VMEM(extra.shape, extra.dtype),
            pltpu.SemaphoreType.DMA((PACK_STEPS + 1,)),
            pltpu.SemaphoreType.DMA((PACK_STEPS + 1,)),
        ],
        name="pack",
    )(samples, extra)


def series(z):
    zz = z * z
    sin = z + z * zz * (
        -1.0 / 6 + zz * (1.0 / 120 + zz * (-1.0 / 5040 + zz * (1.0 / 362880)))
    )
    cos = 1.0 + zz * (
        -0.5 + zz * (1.0 / 24 + zz * (-1.0 / 720 + zz * (1.0 / 40320 + zz * (-1.0 / 3628800))))
    )
    return sin, cos


def turns(angle, lane):
    sin0, cos0 = series(angle * lane)
    sin_h, cos_h = series(angle * (LANES // 2))
    sin1, cos1 = 2.0 * sin_h * cos_h, 1.0 - 2.0 * sin_h * sin_h
    sin2, cos2 = 2.0 * sin1 * cos1, 1.0 - 2.0 * sin1 * sin1
    cc, ss, sc, cs = cos0 * cos1, sin0 * sin1, sin0 * cos1, cos0 * sin1
    return (
        (cos0, sin0),
        (cc - ss, sc + cs),
        (cos0 * cos2 + sin0 * sin2, sin0 * cos2 - cos0 * sin2),
        (cc + ss, sc - cs),
    )


def cells_kernel(
    x_ref, valid_ref, table_ref, second_ref, first_ref, coh_ref, ifg_ref, sums_ref,
    wide_ref, spec_ref, angle_ref, turned_ref, pix_ref, gamma_ref, int_ref,
):
    step = pl.program_id(0)
    dates = first_ref.shape[0]
    date_steps = dates // DATES_STEP
    range_steps = LOOK_RG // COLS_STEP
    stride = wide_ref.shape[0] // DATES_STEP

    @pl.when(step < date_steps)
    def _forward():
        wide_ref[...] = x_ref[...].astype(jnp.float32)
        valid = valid_ref[...]
        shifts = wide_ref[pl.ds(LOOK_RG * COL_ROWS, DATES_STEP, stride=stride), :]
        for c in range(LOOK_RG):
            parts = []
            for part in range(2):
                for block in range(BLOCKS):
                    rows = pl.ds(c * COL_ROWS + 2 * block + part, DATES_STEP, stride=stride)
                    parts.append(
                        (wide_ref[rows, :] * valid[:, block * LANES : (block + 1) * LANES]).astype(
                            jnp.bfloat16
                        )
                    )
            spec_ref[c * DATES_STEP : (c + 1) * DATES_STEP, :] = jnp.concatenate(parts, 1)
            angle_ref[c * DATES_STEP : (c + 1) * DATES_STEP, :] = jnp.broadcast_to(shifts[:, c : c + 1] * (
                -2.0 * math.pi / AZ
            ), (DATES_STEP, LANES))
        spec_ref[...] = jnp.dot(
            spec_ref[...], table_ref[...], preferred_element_type=jnp.float32
        ).astype(jnp.bfloat16)
        lane = lax.broadcasted_iota(jnp.int32, (1, LANES), 1).astype(jnp.float32)
        groups = DATES_STEP // ROT_ROWS

        def turn(i, _):
            rows = pl.ds(pl.multiple_of(i * ROT_ROWS, ROT_ROWS), ROT_ROWS)
            column, group = i // groups, i % groups
            target = pl.ds(
                pl.multiple_of(column * dates + step * DATES_STEP + group * ROT_ROWS, ROT_ROWS),
                ROT_ROWS,
            )
            for block, (cos, sin) in enumerate(turns(angle_ref[rows, :], lane)):
                at = slice(block * LANES, (block + 1) * LANES)
                at_imag = slice(AZ + block * LANES, AZ + (block + 1) * LANES)
                real = spec_ref[rows, at].astype(jnp.float32)
                imag = spec_ref[rows, at_imag].astype(jnp.float32)
                turned_ref[target, at] = (real * cos - imag * sin).astype(jnp.bfloat16)
                turned_ref[target, at_imag] = (real * sin + imag * cos).astype(jnp.bfloat16)
            return _

        lax.fori_loop(0, LOOK_RG * groups, turn, None)

    @pl.when((step >= date_steps) & (step < date_steps + range_steps))
    def _inverse():
        first_column = (step - date_steps) * COLS_STEP
        rows = pl.ds(pl.multiple_of(first_column * dates, COLS_STEP * dates), COLS_STEP * dates)
        restored = lax.dot_general(
            table_ref[...], turned_ref[rows, :], (((1,), (1,)), ((), ())),
            preferred_element_type=jnp.float32,
        )
        restored = (restored * (1.0 / AZ)).astype(jnp.bfloat16)
        for c in range(COLS_STEP):
            pix_ref[:, :, first_column + c] = restored[:, c * dates : (c + 1) * dates].reshape(
                2, LINE_CELLS, LOOK_AZ, dates
            )

    @pl.when(step >= date_steps + range_steps)
    def _covariance():
        diagonal = lax.broadcasted_iota(jnp.int32, (dates, dates), 0) == lax.broadcasted_iota(
            jnp.int32, (dates, dates), 1
        )
        base = (step - date_steps - range_steps) * CELLS_STEP
        for k in range(CELLS_STEP):
            real = pix_ref[0, base + k].reshape(LOOK_RG * LOOK_AZ, dates)
            imag = pix_ref[1, base + k].reshape(LOOK_RG * LOOK_AZ, dates)
            pixels = jnp.concatenate([real, imag], 0)
            partner = jnp.concatenate([pixels, jnp.concatenate([-imag, real], 0)], 1)
            cov = lax.dot_general(
                pixels, partner, (((0,), (0,)), ((), ())), preferred_element_type=jnp.float32
            )
            on_diagonal = jnp.where(diagonal, cov[:, :dates], 0.0)
            scale_rows = lax.rsqrt(jnp.sum(on_diagonal, 1, keepdims=True) + DAMPING)
            scale_cols = lax.rsqrt(jnp.sum(on_diagonal, 0, keepdims=True) + DAMPING)
            scale = scale_rows * scale_cols
            for part in range(2):
                gamma = cov[:, part * dates : (part + 1) * dates] * scale
                high = gamma.astype(jnp.bfloat16)
                coh_ref[k, part] = high
                rows = slice((2 * k + part) * dates, (2 * k + part + 1) * dates)
                gamma_ref[rows, :dates] = high
                gamma_ref[rows, dates:] = (gamma - high.astype(jnp.float32)).astype(jnp.bfloat16)
        picked = jnp.dot(gamma_ref[...], second_ref[...], preferred_element_type=jnp.float32)
        first = first_ref[...]
        for k in range(CELLS_STEP):
            for part in range(2):
                rows = slice((2 * k + part) * dates, (2 * k + part + 1) * dates)
                int_ref[base + k, part : part + 1, :] = jnp.sum(
                    picked[rows] * first, 0, keepdims=True
                )

    @pl.when(step == pl.num_programs(0) - 1)
    def _sums():
        ifg = int_ref[...]
        ifg_ref[...] = ifg
        real, imag = ifg[:, 0, :], ifg[:, 1, :]
        weight = 0.1 + real * real + imag * imag
        line = lax.broadcasted_iota(jnp.int32, (LINE_CELLS, 1), 0).astype(jnp.float32)
        across = (line + 0.5) / LINE_CELLS - 0.5
        tilted = weight * across
        terms = (
            weight, tilted, tilted * across, weight * real, tilted * real, weight * imag, tilted * imag
        )
        for k, term in enumerate(terms):
            sums_ref[k : k + 1, :] = jnp.sum(term, 0, keepdims=True)
        sums_ref[len(terms) :, :] = jnp.zeros_like(sums_ref[len(terms) :, :])


def cells_call(x, valid, table, second, first):
    dates, pairs = first.shape
    date_steps = dates // DATES_STEP
    before = date_steps + LOOK_RG // COLS_STEP
    steps = before + LINE_CELLS // CELLS_STEP
    stride = x.shape[0] // dates
    last = date_steps - 1

    def whole(*shape):
        return pl.BlockSpec(shape, lambda s: (0,) * len(shape))

    return pl.pallas_call(
        cells_kernel,
        grid=(steps,),
        in_specs=[
            pl.BlockSpec((DATES_STEP * stride, LANES), lambda s: (jnp.minimum(s, last), 0)),
            pl.BlockSpec((DATES_STEP, AZ), lambda s: (jnp.minimum(s, last), 0)),
            whole(2 * AZ, 2 * AZ),
            whole(2 * dates, pairs),
            whole(dates, pairs),
        ],
        out_specs=[
            pl.BlockSpec(
                (CELLS_STEP, 2, dates, dates), lambda s: (jnp.maximum(s - before, 0), 0, 0, 0)
            ),
            whole(LINE_CELLS, 2, pairs),
            whole(8, pairs),
        ],
        out_shape=[
            jax.ShapeDtypeStruct((LINE_CELLS, 2, dates, dates), jnp.bfloat16),
            jax.ShapeDtypeStruct((LINE_CELLS, 2, pairs), jnp.float32),
            jax.ShapeDtypeStruct((8, pairs), jnp.float32),
        ],
        scratch_shapes=[
            pltpu.VMEM((DATES_STEP * stride, LANES), jnp.float32),
            pltpu.VMEM((LOOK_RG * DATES_STEP, 2 * AZ), jnp.bfloat16),
            pltpu.VMEM((LOOK_RG * DATES_STEP, LANES), jnp.float32),
            pltpu.VMEM((LOOK_RG * dates, 2 * AZ), jnp.bfloat16),
            pltpu.VMEM((2, LINE_CELLS, LOOK_RG, LOOK_AZ, dates), jnp.bfloat16),
            pltpu.VMEM((2 * CELLS_STEP * dates, 2 * dates), jnp.bfloat16),
            pltpu.VMEM((LINE_CELLS, 2, pairs), jnp.float32),
        ],
        compiler_params=pltpu.CompilerParams(dimension_semantics=("arbitrary",)),
        name="cells",
    )(x, valid, table, second, first)


def line_blocks(samples):
    count, columns = samples.shape[:2]
    blocks = samples.reshape(count, columns, 2, BLOCKS, LANES).transpose(0, 1, 3, 2, 4)
    return blocks.reshape(count, columns * BLOCKS, 2, LANES)


def plane_terms(sums, along):
    w0, w1, w2, r0, r1, i0, i1 = (sums[k] for k in range(7))
    terms = (
        w0, w1, w0 * along, w2, w1 * along, w0 * along * along,
        r0, r1, r0 * along, i0, i1, i0 * along,
    )
    return jnp.stack(terms, 0)


def solve_three(n):
    adjugate_00 = n[3] * n[5] - n[4] * n[4]
    adjugate_01 = n[2] * n[4] - n[1] * n[5]
    adjugate_02 = n[1] * n[4] - n[2] * n[3]
    adjugate_11 = n[0] * n[5] - n[2] * n[2]
    adjugate_12 = n[1] * n[2] - n[0] * n[4]
    adjugate_22 = n[0] * n[3] - n[1] * n[1]
    determinant = n[0] * adjugate_00 + n[1] * adjugate_01 + n[2] * adjugate_02
    parts = []
    for t in (n[6:9], n[9:12]):
        parts.append(
            jnp.stack(
                [
                    adjugate_00 * t[0] + adjugate_01 * t[1] + adjugate_02 * t[2],
                    adjugate_01 * t[0] + adjugate_11 * t[1] + adjugate_12 * t[2],
                    adjugate_02 * t[0] + adjugate_12 * t[1] + adjugate_22 * t[2],
                ],
                0,
            )
            / determinant
        )
    return jnp.stack(parts, 0)


def summed_over(array, axis):
    copies = jnp.broadcast_to(array[None], (lax.axis_size(axis), *array.shape))
    return jnp.sum(lax.all_to_all(copies, axis, 0, 0, tiled=True), 0)


def along_of(position, range_cells):
    return (position.astype(jnp.float32) + 0.5) / range_cells - 0.5


def fitted(sums, range_cells):
    core = lax.axis_index("wide_2")
    position = lax.axis_index(WIDE)
    other = position + 1 - 2 * core
    swap = [(0, 1), (1, 0)]
    halves = sums.reshape(sums.shape[0], 2, -1)
    keep = jnp.where(core == 0, halves[:, 0], halves[:, 1])
    give = jnp.where(core == 0, halves[:, 1], halves[:, 0])
    got = lax.ppermute(give, "wide_2", swap)
    terms = plane_terms(keep, along_of(position, range_cells)) + plane_terms(
        got, along_of(other, range_cells)
    )
    ramps = solve_three(summed_over(summed_over(terms, "wide_1"), "wide_0"))
    others = lax.ppermute(ramps, "wide_2", swap)
    return jnp.where(
        core == 0, jnp.concatenate([ramps, others], -1), jnp.concatenate([others, ramps], -1)
    )


def local(slc, offsets, row_start, row_stop, pairs):
    devices = lax.axis_size(WIDE)
    position = lax.axis_index(WIDE)
    columns = slc.shape[1]
    here = columns // devices
    dates = devices * slc.shape[0]
    extra = jnp.pad(offsets.reshape(devices, 1, 1, here), ((0, 0), (0, 0), (0, 1), (0, LANES - here)))
    sent = packed(line_blocks(slc.reshape(devices, here, 2, AZ)), extra)
    received = lax.all_to_all(sent, WIDE, 0, 0, tiled=True)
    lines = jnp.arange(AZ, dtype=jnp.int32)[None, :]
    valid = ((lines >= row_start[:, None]) & (lines < row_stop[:, None])).astype(jnp.float32)
    date = jnp.arange(dates, dtype=jnp.int32)[:, None]
    first = (date == pairs[:, 0][None, :]).astype(jnp.float32)
    second = (date == pairs[:, 1][None, :]).astype(jnp.bfloat16)
    second = jnp.concatenate([second, second], 0)
    coherence, ifg, sums = cells_call(
        received.reshape(-1, LANES), valid, spectral_table(), second, first
    )

    range_cells = columns // LOOK_RG
    ramps = fitted(sums, range_cells)
    share = pairs.shape[0] // devices
    own = lax.dynamic_slice_in_dim(ramps, position * share, share, 2).transpose(2, 0, 1)
    across = (jnp.arange(LINE_CELLS, dtype=jnp.int32).astype(jnp.float32) + 0.5) / LINE_CELLS - 0.5
    along = along_of(position, range_cells)
    plane = ramps[:, 0] + across[:, None, None] * ramps[:, 1] + along * ramps[:, 2]
    return coherence, ifg - plane, own


def solution(mesh):
    torus = Mesh(
        mesh.devices.reshape(mesh.shape["slab"], 8, 8, 2), ("slab", "wide_0", "wide_1", "wide_2")
    )
    in_specs = (P(WIDE, "slab", None, None), P(WIDE, "slab"), P(), P(), P())
    out_specs = (P(SLAB_WIDE, None, None, None), P(SLAB_WIDE, None, None), P(SLAB_WIDE, None, None))
    return jax.shard_map(local, mesh=torus, in_specs=in_specs, out_specs=out_specs, check_vma=False)
```

```python
import math

import jax
import jax.numpy as jnp
from jax import lax
from jax.experimental import pallas as pl
from jax.experimental.pallas import tpu as pltpu
from jax.sharding import Mesh
from jax.sharding import PartitionSpec as P

AZ = 512
LOOK_AZ = 16
LOOK_RG = 16
LINE_CELLS = AZ // LOOK_AZ
WIDE = ("wide_0", "wide_1", "wide_2")
SLAB_WIDE = ("slab", "wide_0", "wide_1", "wide_2")
DAMPING = 1.0
DATES_STEP = 32
COLS_STEP = 8
CELLS_STEP = 8
ROT_ROWS = 32
LANES = 128
BLOCKS = AZ // LANES
HALF = AZ // 2
COL_ROWS = 2 * BLOCKS
PACK_STEPS = 4


def bins_of(odd):
    j = 2 * jnp.arange(HALF // 2, dtype=jnp.int32) + odd
    return jnp.concatenate([j, jnp.where(j == 0, AZ // 2, AZ - j)], 0)


def spectral_tables():
    line = jnp.arange(HALF, dtype=jnp.int32)[:, None]
    tables = []
    for odd in range(2):
        angles = (line * bins_of(odd)[None, :] % AZ).astype(jnp.float32) * (2.0 * math.pi / AZ)
        cosine = jnp.cos(angles).astype(jnp.bfloat16)
        sine = jnp.sin(angles).astype(jnp.bfloat16)
        tables.append(
            jnp.concatenate(
                [jnp.concatenate([cosine, -sine], 1), jnp.concatenate([sine, cosine], 1)], 0
            )
        )
    return jnp.stack(tables, 0)


def pack_kernel(samples_ref, offsets_ref, out_ref, buffer, own, extra_buffer, in_sem, out_sem):
    devices, width = samples_ref.shape[:2]
    share = devices // PACK_STEPS
    rows = [pl.ds(i * share, share) for i in range(PACK_STEPS)]
    ins = [
        pltpu.make_async_copy(samples_ref.at[rows[i]], buffer.at[rows[i]], in_sem.at[i])
        for i in range(PACK_STEPS)
    ]
    outs = [
        pltpu.make_async_copy(
            buffer.at[rows[i]], out_ref.at[rows[i], pl.ds(0, width)], out_sem.at[i]
        )
        for i in range(PACK_STEPS)
    ]
    own_in = pltpu.make_async_copy(offsets_ref, own, in_sem.at[PACK_STEPS])
    own_in.start()
    for copy in ins:
        copy.start()
    own_in.wait()
    sharing = devices * LANES // offsets_ref.shape[1]
    for k in range(devices // sharing):
        block = jnp.broadcast_to(own[:, k * LANES : (k + 1) * LANES], (2, LANES))
        for i in range(sharing):
            extra_buffer[k * sharing + i, 0] = block
    extra = pltpu.make_async_copy(
        extra_buffer, out_ref.at[:, pl.ds(width, 1)], out_sem.at[PACK_STEPS]
    )
    extra.start()
    for copy_in, copy_out in zip(ins, outs):
        copy_in.wait()
        copy_out.start()
    extra.wait()
    for copy in outs:
        copy.wait()


def packed(samples, offsets):
    devices, width = samples.shape[:2]
    return pl.pallas_call(
        pack_kernel,
        in_specs=[pl.BlockSpec(memory_space=pl.ANY)] * 2,
        out_specs=pl.BlockSpec(memory_space=pl.ANY),
        out_shape=jax.ShapeDtypeStruct((devices, width + 1, 2, LANES), samples.dtype),
        scratch_shapes=[
            pltpu.VMEM(samples.shape, samples.dtype),
            pltpu.VMEM(offsets.shape, offsets.dtype),
            pltpu.VMEM((devices, 1, 2, LANES), samples.dtype),
            pltpu.SemaphoreType.DMA((PACK_STEPS + 1,)),
            pltpu.SemaphoreType.DMA((PACK_STEPS + 1,)),
        ],
        name="pack",
    )(samples, offsets)


def series(z):
    zz = z * z
    sin = z + z * zz * (
        -1.0 / 6 + zz * (1.0 / 120 + zz * (-1.0 / 5040 + zz * (1.0 / 362880)))
    )
    cos = 1.0 + zz * (
        -0.5 + zz * (1.0 / 24 + zz * (-1.0 / 720 + zz * (1.0 / 40320 + zz * (-1.0 / 3628800))))
    )
    return cos, sin


def turns(angle, lane):
    cos, sin = series(angle * jnp.where(lane == 0.0, HALF / 2.0, lane))
    cos, sin = 1.0 - 2.0 * sin * sin, 2.0 * sin * cos
    even_cos, even_sin = jnp.where(lane == 0.0, 1.0, cos), jnp.where(lane == 0.0, 0.0, sin)
    square = angle * angle
    one_cos, one_sin = 1.0 - square * (0.5 - square * (1.0 / 24)), angle - angle * square * (1.0 / 6)
    odd_cos = even_cos * one_cos - even_sin * one_sin
    odd_sin = even_cos * one_sin + even_sin * one_cos
    return (even_cos, even_sin), (cos, -sin), (odd_cos, odd_sin), (odd_cos, -odd_sin)


def cells_kernel(
    at_ref, x_ref, valid_ref, table_ref, second_ref, first_ref, coh_ref, ifg_ref, sums_ref,
    wide_ref, spec_ref, angle_ref, turned_ref, pix_ref, gamma_ref, int_ref,
):
    step = pl.program_id(0)
    dates = first_ref.shape[0]
    date_steps = dates // DATES_STEP
    range_steps = LOOK_RG // COLS_STEP
    stride = wide_ref.shape[0] // DATES_STEP

    @pl.when(step < date_steps)
    def _forward():
        wide_ref[...] = x_ref[...].astype(jnp.float32)
        valid = valid_ref[...]
        shifts = wide_ref[pl.ds(LOOK_RG * COL_ROWS, DATES_STEP, stride=stride), :]
        shifts = pltpu.roll(shifts, at_ref[0], 1)
        for c in range(LOOK_RG):
            sums, differences = [], []
            for part in range(2):
                for block in range(BLOCKS // 2):
                    low, high = (
                        wide_ref[pl.ds(c * COL_ROWS + 2 * b + part, DATES_STEP, stride=stride), :]
                        * valid[:, b * LANES : (b + 1) * LANES]
                        for b in (block, block + BLOCKS // 2)
                    )
                    sums.append((low + high).astype(jnp.bfloat16))
                    differences.append((low - high).astype(jnp.bfloat16))
            rows = slice(c * DATES_STEP, (c + 1) * DATES_STEP)
            spec_ref[rows, :] = jnp.concatenate(sums + differences, 1)
            angle_ref[rows, :] = jnp.broadcast_to(
                shifts[:, c : c + 1] * (-2.0 * math.pi / AZ), (DATES_STEP, LANES)
            )
        for odd in range(2):
            at = slice(odd * AZ, (odd + 1) * AZ)
            spec_ref[:, at] = jnp.dot(
                spec_ref[:, at], table_ref[odd], preferred_element_type=jnp.float32
            ).astype(jnp.bfloat16)
        lane = lax.broadcasted_iota(jnp.int32, (1, LANES), 1).astype(jnp.float32)
        groups = DATES_STEP // ROT_ROWS

        def turn(i, _):
            rows = pl.ds(pl.multiple_of(i * ROT_ROWS, ROT_ROWS), ROT_ROWS)
            column, group = i // groups, i % groups
            target = pl.ds(
                pl.multiple_of(column * dates + step * DATES_STEP + group * ROT_ROWS, ROT_ROWS),
                ROT_ROWS,
            )
            for block, (cos, sin) in enumerate(turns(angle_ref[rows, :], lane)):
                start = (block // 2) * AZ + (block % 2) * LANES
                at, at_imag = slice(start, start + LANES), slice(start + HALF, start + HALF + LANES)
                real = spec_ref[rows, at].astype(jnp.float32)
                imag = spec_ref[rows, at_imag].astype(jnp.float32)
                turned_ref[target, at] = (real * cos - imag * sin).astype(jnp.bfloat16)
                turned_ref[target, at_imag] = (real * sin + imag * cos).astype(jnp.bfloat16)
            return _

        lax.fori_loop(0, LOOK_RG * groups, turn, None)

    @pl.when((step >= date_steps) & (step < date_steps + range_steps))
    def _inverse():
        first_column = (step - date_steps) * COLS_STEP
        rows = pl.ds(pl.multiple_of(first_column * dates, COLS_STEP * dates), COLS_STEP * dates)
        even, odd = (
            lax.dot_general(
                table_ref[k], turned_ref[rows, k * AZ : (k + 1) * AZ], (((1,), (1,)), ((), ())),
                preferred_element_type=jnp.float32,
            )
            for k in range(2)
        )
        for half, restored in enumerate((even + odd, even - odd)):
            restored = (restored * (1.0 / AZ)).astype(jnp.bfloat16)
            cells = slice(half * LINE_CELLS // 2, (half + 1) * LINE_CELLS // 2)
            for c in range(COLS_STEP):
                pix_ref[:, cells, first_column + c] = restored[
                    :, c * dates : (c + 1) * dates
                ].reshape(2, LINE_CELLS // 2, LOOK_AZ, dates)

    @pl.when(step >= date_steps + range_steps)
    def _covariance():
        diagonal = lax.broadcasted_iota(jnp.int32, (dates, dates), 0) == lax.broadcasted_iota(
            jnp.int32, (dates, dates), 1
        )
        base = (step - date_steps - range_steps) * CELLS_STEP
        for k in range(CELLS_STEP):
            real = pix_ref[0, base + k].reshape(LOOK_RG * LOOK_AZ, dates)
            imag = pix_ref[1, base + k].reshape(LOOK_RG * LOOK_AZ, dates)
            pixels = jnp.concatenate([real, imag], 0)
            partner = jnp.concatenate([pixels, jnp.concatenate([-imag, real], 0)], 1)
            cov = lax.dot_general(
                pixels, partner, (((0,), (0,)), ((), ())), preferred_element_type=jnp.float32
            )
            on_diagonal = jnp.where(diagonal, cov[:, :dates], 0.0)
            scale_rows = lax.rsqrt(jnp.sum(on_diagonal, 1, keepdims=True) + DAMPING)
            scale_cols = lax.rsqrt(jnp.sum(on_diagonal, 0, keepdims=True) + DAMPING)
            scale = scale_rows * scale_cols
            for part in range(2):
                gamma = cov[:, part * dates : (part + 1) * dates] * scale
                high = gamma.astype(jnp.bfloat16)
                coh_ref[k, part] = high
                rows = slice((2 * k + part) * dates, (2 * k + part + 1) * dates)
                gamma_ref[rows, :dates] = high
                gamma_ref[rows, dates:] = (gamma - high.astype(jnp.float32)).astype(jnp.bfloat16)
        picked = jnp.dot(gamma_ref[...], second_ref[...], preferred_element_type=jnp.float32)
        first = first_ref[...]
        for k in range(CELLS_STEP):
            for part in range(2):
                rows = slice((2 * k + part) * dates, (2 * k + part + 1) * dates)
                int_ref[base + k, part : part + 1, :] = jnp.sum(
                    picked[rows] * first, 0, keepdims=True
                )

    @pl.when(step == pl.num_programs(0) - 1)
    def _sums():
        ifg = int_ref[...]
        ifg_ref[...] = ifg
        real, imag = ifg[:, 0, :], ifg[:, 1, :]
        weight = 0.1 + real * real + imag * imag
        line = lax.broadcasted_iota(jnp.int32, (LINE_CELLS, 1), 0).astype(jnp.float32)
        across = (line + 0.5) / LINE_CELLS - 0.5
        tilted = weight * across
        terms = (
            weight, tilted, tilted * across, weight * real, tilted * real, weight * imag, tilted * imag
        )
        for k, term in enumerate(terms):
            sums_ref[k : k + 1, :] = jnp.sum(term, 0, keepdims=True)
        sums_ref[len(terms) :, :] = jnp.zeros_like(sums_ref[len(terms) :, :])


def cells_call(at, x, valid, table, second, first):
    dates, pairs = first.shape
    date_steps = dates // DATES_STEP
    before = date_steps + LOOK_RG // COLS_STEP
    steps = before + LINE_CELLS // CELLS_STEP
    stride = x.shape[0] // dates
    last = date_steps - 1

    def whole(*shape):
        return pl.BlockSpec(shape, lambda s: (0,) * len(shape))

    return pl.pallas_call(
        cells_kernel,
        grid=(steps,),
        in_specs=[
            pl.BlockSpec(memory_space=pltpu.SMEM),
            pl.BlockSpec((DATES_STEP * stride, LANES), lambda s: (jnp.minimum(s, last), 0)),
            pl.BlockSpec((DATES_STEP, AZ), lambda s: (jnp.minimum(s, last), 0)),
            pl.BlockSpec(memory_space=pltpu.VMEM),
            pl.BlockSpec(memory_space=pltpu.VMEM),
            pl.BlockSpec(memory_space=pltpu.VMEM),
        ],
        out_specs=[
            pl.BlockSpec(
                (CELLS_STEP, 2, dates, dates), lambda s: (jnp.maximum(s - before, 0), 0, 0, 0)
            ),
            whole(LINE_CELLS, 2, pairs),
            whole(8, pairs),
        ],
        out_shape=[
            jax.ShapeDtypeStruct((LINE_CELLS, 2, dates, dates), jnp.bfloat16),
            jax.ShapeDtypeStruct((LINE_CELLS, 2, pairs), jnp.float32),
            jax.ShapeDtypeStruct((8, pairs), jnp.float32),
        ],
        scratch_shapes=[
            pltpu.VMEM((DATES_STEP * stride, LANES), jnp.float32),
            pltpu.VMEM((LOOK_RG * DATES_STEP, 2 * AZ), jnp.bfloat16),
            pltpu.VMEM((LOOK_RG * DATES_STEP, LANES), jnp.float32),
            pltpu.VMEM((LOOK_RG * dates, 2 * AZ), jnp.bfloat16),
            pltpu.VMEM((2, LINE_CELLS, LOOK_RG, LOOK_AZ, dates), jnp.bfloat16),
            pltpu.VMEM((2 * CELLS_STEP * dates, 2 * dates), jnp.bfloat16),
            pltpu.VMEM((LINE_CELLS, 2, pairs), jnp.float32),
        ],
        compiler_params=pltpu.CompilerParams(
            dimension_semantics=("arbitrary",), vmem_limit_bytes=48 * 1024 * 1024
        ),
        name="cells",
    )(at, x, valid, table, second, first)


def line_blocks(samples):
    count, columns = samples.shape[:2]
    blocks = samples.reshape(count, columns, 2, BLOCKS, LANES).transpose(0, 1, 3, 2, 4)
    return blocks.reshape(count, columns * BLOCKS, 2, LANES)


def plane_terms(sums, along):
    w0, w1, w2, r0, r1, i0, i1 = (sums[k] for k in range(7))
    terms = (
        w0, w1, w0 * along, w2, w1 * along, w0 * along * along,
        r0, r1, r0 * along, i0, i1, i0 * along,
    )
    return jnp.stack(terms, 0)


def solve_three(n):
    adjugate_00 = n[3] * n[5] - n[4] * n[4]
    adjugate_01 = n[2] * n[4] - n[1] * n[5]
    adjugate_02 = n[1] * n[4] - n[2] * n[3]
    adjugate_11 = n[0] * n[5] - n[2] * n[2]
    adjugate_12 = n[1] * n[2] - n[0] * n[4]
    adjugate_22 = n[0] * n[3] - n[1] * n[1]
    determinant = n[0] * adjugate_00 + n[1] * adjugate_01 + n[2] * adjugate_02
    parts = []
    for t in (n[6:9], n[9:12]):
        parts.append(
            jnp.stack(
                [
                    adjugate_00 * t[0] + adjugate_01 * t[1] + adjugate_02 * t[2],
                    adjugate_01 * t[0] + adjugate_11 * t[1] + adjugate_12 * t[2],
                    adjugate_02 * t[0] + adjugate_12 * t[1] + adjugate_22 * t[2],
                ],
                0,
            )
            / determinant
        )
    return jnp.stack(parts, 0)


def summed_over(array, axis):
    copies = jnp.broadcast_to(array[None], (lax.axis_size(axis), *array.shape))
    return jnp.sum(lax.all_to_all(copies, axis, 0, 0, tiled=True), 0)


def along_of(position, range_cells):
    return (position.astype(jnp.float32) + 0.5) / range_cells - 0.5


def fitted(sums, range_cells):
    core = lax.axis_index("wide_2")
    position = lax.axis_index(WIDE)
    other = position + 1 - 2 * core
    swap = [(0, 1), (1, 0)]
    halves = sums.reshape(sums.shape[0], 2, -1)
    keep = jnp.where(core == 0, halves[:, 0], halves[:, 1])
    give = jnp.where(core == 0, halves[:, 1], halves[:, 0])
    got = lax.ppermute(give, "wide_2", swap)
    terms = plane_terms(keep, along_of(position, range_cells)) + plane_terms(
        got, along_of(other, range_cells)
    )
    ramps = solve_three(summed_over(summed_over(terms, "wide_1"), "wide_0"))
    others = lax.ppermute(ramps, "wide_2", swap)
    return jnp.where(
        core == 0, jnp.concatenate([ramps, others], -1), jnp.concatenate([others, ramps], -1)
    )


def local(slc, offsets, row_start, row_stop, pairs):
    devices = lax.axis_size(WIDE)
    position = lax.axis_index(WIDE)
    columns = slc.shape[1]
    here = columns // devices
    dates = devices * slc.shape[0]
    at = (LANES - here * (position % (LANES // here))) % LANES
    sent = packed(line_blocks(slc.reshape(devices, here, 2, AZ)), offsets)
    received = lax.all_to_all(sent, WIDE, 0, 0, tiled=True)
    lines = jnp.arange(AZ, dtype=jnp.int32)[None, :]
    valid = ((lines >= row_start[:, None]) & (lines < row_stop[:, None])).astype(jnp.float32)
    date = jnp.arange(dates, dtype=jnp.int32)[:, None]
    first = (date == pairs[:, 0][None, :]).astype(jnp.float32)
    second = (date == pairs[:, 1][None, :]).astype(jnp.bfloat16)
    second = jnp.concatenate([second, second], 0)
    coherence, ifg, sums = cells_call(
        at.reshape(1), received.reshape(-1, LANES), valid, spectral_tables(), second, first
    )

    range_cells = columns // LOOK_RG
    ramps = fitted(sums, range_cells)
    share = pairs.shape[0] // devices
    own = lax.dynamic_slice_in_dim(ramps, position * share, share, 2).transpose(2, 0, 1)
    across = (jnp.arange(LINE_CELLS, dtype=jnp.int32).astype(jnp.float32) + 0.5) / LINE_CELLS - 0.5
    along = along_of(position, range_cells)
    plane = ramps[:, 0] + across[:, None, None] * ramps[:, 1] + along * ramps[:, 2]
    return coherence, ifg - plane, own


def solution(mesh):
    torus = Mesh(
        mesh.devices.reshape(mesh.shape["slab"], 8, 8, 2), ("slab", "wide_0", "wide_1", "wide_2")
    )
    in_specs = (P(WIDE, "slab", None, None), P(WIDE, "slab"), P(), P(), P())
    out_specs = (P(SLAB_WIDE, None, None, None), P(SLAB_WIDE, None, None), P(SLAB_WIDE, None, None))
    return jax.shard_map(local, mesh=torus, in_specs=in_specs, out_specs=out_specs, check_vma=False)
```

```python
import functools
import math

import jax
import jax.numpy as jnp
from jax import lax
from jax.experimental import pallas as pl
from jax.experimental.pallas import tpu as pltpu
from jax.sharding import Mesh
from jax.sharding import PartitionSpec as P

AZ = 512
LOOK_AZ = 16
LOOK_RG = 16
LINE_CELLS = AZ // LOOK_AZ
WIDE = ("wide_0", "wide_1", "wide_2")
SLAB_WIDE = ("slab", "wide_0", "wide_1", "wide_2")
SEND = ("wide_1", "wide_0", "wide_2")
DAMPING = 1.0
DATES_STEP = 32
COLS_STEP = 8
CELLS_STEP = 8
LANES = 128
BLOCKS = AZ // LANES
HALF = AZ // 2
SCALE = 1.0 / AZ
COL_ROWS = 2 * BLOCKS
SUBLANES = 8


def bins_of(odd):
    j = 2 * jnp.arange(HALF // 2, dtype=jnp.int32) + odd
    return jnp.concatenate([j, jnp.where(j == 0, AZ // 2, AZ - j)], 0)


def spectral_tables():
    line = jnp.arange(HALF, dtype=jnp.int32)[:, None]
    tables = []
    for odd in range(2):
        angles = (line * bins_of(odd)[None, :] % AZ).astype(jnp.float32) * (2.0 * math.pi / AZ)
        cosine = jnp.cos(angles).astype(jnp.bfloat16)
        sine = jnp.sin(angles).astype(jnp.bfloat16)
        tables.append(
            jnp.concatenate(
                [jnp.concatenate([cosine, -sine], 1), jnp.concatenate([sine, cosine], 1)], 0
            )
        )
    return jnp.stack(tables, 0)


def pack_kernel(samples_ref, offsets_ref, out_ref, buffer, own, extra_buffer, in_sem, out_sem):
    major, minor, cores, width = samples_ref.shape[:4]
    ins = [
        pltpu.make_async_copy(samples_ref.at[:, i], buffer.at[i], in_sem.at[i])
        for i in range(minor)
    ]
    outs = [
        pltpu.make_async_copy(buffer.at[i], out_ref.at[i, :, :, pl.ds(0, width)], out_sem.at[i])
        for i in range(minor)
    ]
    own_in = pltpu.make_async_copy(offsets_ref, own, in_sem.at[minor])
    own_in.start()
    for copy in ins:
        copy.start()
    own_in.wait()
    here = offsets_ref.shape[1] // (major * minor * cores)
    for x in range(major):
        for y in range(minor):
            for core in range(cores):
                start = ((x * minor + y) * cores + core) * here // LANES * LANES
                extra_buffer[y, x, core, 0] = jnp.broadcast_to(
                    own[:, start : start + LANES], (2, LANES)
                )
    extra = pltpu.make_async_copy(
        extra_buffer, out_ref.at[:, :, :, pl.ds(width, 1)], out_sem.at[minor]
    )
    extra.start()
    for copy_in, copy_out in zip(ins, outs):
        copy_in.wait()
        copy_out.start()
    extra.wait()
    for copy in outs:
        copy.wait()


def packed(samples, offsets):
    major, minor, cores, width = samples.shape[:4]
    return pl.pallas_call(
        pack_kernel,
        in_specs=[pl.BlockSpec(memory_space=pl.ANY)] * 2,
        out_specs=pl.BlockSpec(memory_space=pl.ANY),
        out_shape=jax.ShapeDtypeStruct((minor, major, cores, width + 1, 2, LANES), samples.dtype),
        scratch_shapes=[
            pltpu.VMEM((minor, major, cores, width, 2, LANES), samples.dtype),
            pltpu.VMEM(offsets.shape, offsets.dtype),
            pltpu.VMEM((minor, major, cores, 1, 2, LANES), samples.dtype),
            pltpu.SemaphoreType.DMA((minor + 1,)),
            pltpu.SemaphoreType.DMA((minor + 1,)),
        ],
        name="pack",
    )(samples, offsets)


def series(z):
    zz = z * z
    sin = z + z * zz * (
        -1.0 / 6 + zz * (1.0 / 120 + zz * (-1.0 / 5040 + zz * (1.0 / 362880)))
    )
    cos = 1.0 + zz * (
        -0.5 + zz * (1.0 / 24 + zz * (-1.0 / 720 + zz * (1.0 / 40320 + zz * (-1.0 / 3628800))))
    )
    return cos, sin


def turns(angle, lane):
    cos, sin = series(angle * jnp.where(lane == 0.0, HALF / 2.0, lane))
    cos, sin = SCALE - (2.0 * SCALE) * sin * sin, (2.0 * SCALE) * sin * cos
    even_cos, even_sin = jnp.where(lane == 0.0, SCALE, cos), jnp.where(lane == 0.0, 0.0, sin)
    square = angle * angle
    one_cos, one_sin = 1.0 - square * (0.5 - square * (1.0 / 24)), angle - angle * square * (1.0 / 6)
    odd_cos = even_cos * one_cos - even_sin * one_sin
    odd_sin = even_cos * one_sin + even_sin * one_cos
    return (even_cos, even_sin), (cos, -sin), (odd_cos, odd_sin), (odd_cos, -odd_sin)


def cells_kernel(
    major, cores, at_ref, x_ref, valid_ref, table_ref, second_ref, first_ref, coh_ref, ifg_ref, sums_ref,
    wide_ref, spec_ref, angle_ref, turned_ref, pix_ref, gamma_ref, int_ref,
):
    step = pl.program_id(0)
    dates = first_ref.shape[0]
    date_steps = dates // DATES_STEP
    range_steps = LOOK_RG // COLS_STEP
    stride = wide_ref.shape[0] // DATES_STEP

    @pl.when(step < date_steps)
    def _forward():
        wide_ref[...] = x_ref[...].astype(jnp.float32)
        valid = valid_ref[...]

        def rows_of(offset):
            return jnp.concatenate(
                [
                    wide_ref[
                        pl.ds((y * major * cores + core) * stride + offset, major, stride=cores * stride), :
                    ]
                    for y in range(DATES_STEP // (major * cores))
                    for core in range(cores)
                ],
                0,
            )

        shifts = rows_of(LOOK_RG * COL_ROWS)
        shifts = pltpu.roll(shifts, at_ref[0], 1)
        for c in range(LOOK_RG):
            sums, differences = [], []
            for part in range(2):
                for block in range(BLOCKS // 2):
                    low, high = (
                        rows_of(c * COL_ROWS + 2 * b + part)
                        * valid[:, b * LANES : (b + 1) * LANES]
                        for b in (block, block + BLOCKS // 2)
                    )
                    sums.append((low + high).astype(jnp.bfloat16))
                    differences.append((low - high).astype(jnp.bfloat16))
            rows = slice(c * DATES_STEP, (c + 1) * DATES_STEP)
            spec_ref[rows, :] = jnp.concatenate(sums + differences, 1)
            angle_ref[rows, :] = jnp.broadcast_to(
                shifts[:, c : c + 1] * (-2.0 * math.pi / AZ), (DATES_STEP, LANES)
            )
        for odd in range(2):
            at = slice(odd * AZ, (odd + 1) * AZ)
            spec_ref[:, at] = jnp.dot(
                spec_ref[:, at], table_ref[odd], preferred_element_type=jnp.float32
            ).astype(jnp.bfloat16)
        lane = lax.broadcasted_iota(jnp.int32, (1, LANES), 1).astype(jnp.float32)

        def turn(column, _):
            rows = pl.ds(pl.multiple_of(column * DATES_STEP, DATES_STEP), DATES_STEP)
            first_row = column * dates + step * (DATES_STEP // major)
            for block, (cos, sin) in enumerate(turns(angle_ref[rows, :], lane)):
                start = (block // 2) * AZ + (block % 2) * LANES
                at, at_imag = slice(start, start + LANES), slice(start + HALF, start + HALF + LANES)
                real = spec_ref[rows, at].astype(jnp.float32)
                imag = spec_ref[rows, at_imag].astype(jnp.float32)
                turned_real, turned_imag = real * cos - imag * sin, real * sin + imag * cos
                for k in range(DATES_STEP // major):
                    for first_lane, turned in ((start, turned_real), (start + HALF, turned_imag)):
                        row = first_lane // LANES * (LOOK_RG * dates) + first_row + k
                        turned_ref[pl.ds(row, major, stride=dates // major), :] = turned[
                            k * major : (k + 1) * major
                        ]
            return _

        lax.fori_loop(0, LOOK_RG, turn, None)

    @pl.when((step >= date_steps) & (step < date_steps + range_steps))
    def _inverse():
        first_column = (step - date_steps) * COLS_STEP

        def turned_rows(block):
            start = block * (LOOK_RG * dates) + first_column * dates
            rows = pl.ds(pl.multiple_of(start, COLS_STEP * dates), COLS_STEP * dates)
            return turned_ref[rows, :].astype(jnp.bfloat16)

        even, odd = (
            lax.dot_general(
                table_ref[k],
                jnp.concatenate([turned_rows(k * BLOCKS + b) for b in range(BLOCKS)], 1),
                (((1,), (1,)), ((), ())),
                preferred_element_type=jnp.float32,
            )
            for k in range(2)
        )
        for half, restored in enumerate((even + odd, even - odd)):
            restored = restored.astype(jnp.bfloat16)
            cells = slice(half * LINE_CELLS // 2, (half + 1) * LINE_CELLS // 2)
            for c in range(COLS_STEP):
                pix_ref[:, cells, first_column + c] = restored[
                    :, c * dates : (c + 1) * dates
                ].reshape(2, LINE_CELLS // 2, LOOK_AZ, dates)

    @pl.when(step >= date_steps + range_steps)
    def _covariance():
        diagonal = lax.broadcasted_iota(jnp.int32, (dates, dates), 0) == lax.broadcasted_iota(
            jnp.int32, (dates, dates), 1
        )
        base = (step - date_steps - range_steps) * CELLS_STEP
        for k in range(CELLS_STEP):
            real = pix_ref[0, base + k].reshape(LOOK_RG * LOOK_AZ, dates)
            imag = pix_ref[1, base + k].reshape(LOOK_RG * LOOK_AZ, dates)
            pixels = jnp.concatenate([real, imag], 0)
            partner = jnp.concatenate([pixels, jnp.concatenate([-imag, real], 0)], 1)
            cov = lax.dot_general(
                pixels, partner, (((0,), (0,)), ((), ())), preferred_element_type=jnp.float32
            )
            on_diagonal = jnp.where(diagonal, cov[:, :dates], 0.0)
            scale_rows = lax.rsqrt(jnp.sum(on_diagonal, 1, keepdims=True) + DAMPING)
            scale_cols = lax.rsqrt(jnp.sum(on_diagonal, 0, keepdims=True) + DAMPING)
            scale = scale_rows * scale_cols
            for part in range(2):
                gamma = cov[:, part * dates : (part + 1) * dates] * scale
                high = gamma.astype(jnp.bfloat16)
                coh_ref[k, part] = high
                rows = slice((2 * k + part) * dates, (2 * k + part + 1) * dates)
                gamma_ref[rows, :] = high
        picked = jnp.dot(gamma_ref[...], second_ref[...], preferred_element_type=jnp.float32)
        first = first_ref[...]
        for k in range(CELLS_STEP):
            for part in range(2):
                rows = slice((2 * k + part) * dates, (2 * k + part + 1) * dates)
                int_ref[base + k, part : part + 1, :] = jnp.sum(
                    picked[rows] * first, 0, keepdims=True
                )

    @pl.when(step == pl.num_programs(0) - 1)
    def _sums():
        ifg = int_ref[...]
        ifg_ref[...] = ifg
        real, imag = ifg[:, 0, :], ifg[:, 1, :]
        weight = 0.1 + real * real + imag * imag
        line = lax.broadcasted_iota(jnp.int32, (LINE_CELLS, 1), 0).astype(jnp.float32)
        across = (line + 0.5) / LINE_CELLS - 0.5
        tilted = weight * across
        terms = (
            weight, tilted, tilted * across, weight * real, tilted * real, weight * imag, tilted * imag
        )
        for k, term in enumerate(terms):
            sums_ref[k : k + 1, :] = jnp.sum(term, 0, keepdims=True)
        sums_ref[len(terms) :, :] = jnp.zeros_like(sums_ref[len(terms) :, :])


def cells_call(major, cores, at, x, valid, table, second, first):
    dates, pairs = first.shape
    date_steps = dates // DATES_STEP
    before = date_steps + LOOK_RG // COLS_STEP
    steps = before + LINE_CELLS // CELLS_STEP
    stride = x.shape[0] // dates
    last = date_steps - 1

    def whole(*shape):
        return pl.BlockSpec(shape, lambda s: (0,) * len(shape))

    return pl.pallas_call(
        functools.partial(cells_kernel, major, cores),
        grid=(steps,),
        in_specs=[
            pl.BlockSpec(memory_space=pltpu.SMEM),
            pl.BlockSpec((DATES_STEP * stride, LANES), lambda s: (jnp.minimum(s, last), 0)),
            pl.BlockSpec((DATES_STEP, AZ), lambda s: (jnp.minimum(s, last), 0)),
            pl.BlockSpec(memory_space=pltpu.VMEM),
            pl.BlockSpec(memory_space=pltpu.VMEM),
            pl.BlockSpec(memory_space=pltpu.VMEM),
        ],
        out_specs=[
            pl.BlockSpec(
                (CELLS_STEP, 2, dates, dates), lambda s: (jnp.maximum(s - before, 0), 0, 0, 0)
            ),
            whole(LINE_CELLS, 2, pairs),
            whole(8, pairs),
        ],
        out_shape=[
            jax.ShapeDtypeStruct((LINE_CELLS, 2, dates, dates), jnp.bfloat16),
            jax.ShapeDtypeStruct((LINE_CELLS, 2, pairs), jnp.float32),
            jax.ShapeDtypeStruct((8, pairs), jnp.float32),
        ],
        scratch_shapes=[
            pltpu.VMEM((DATES_STEP * stride, LANES), jnp.float32),
            pltpu.VMEM((LOOK_RG * DATES_STEP, 2 * AZ), jnp.bfloat16),
            pltpu.VMEM((LOOK_RG * DATES_STEP, LANES), jnp.float32),
            pltpu.VMEM((2 * BLOCKS * LOOK_RG * dates, LANES), jnp.float32),
            pltpu.VMEM((2, LINE_CELLS, LOOK_RG, LOOK_AZ, dates), jnp.bfloat16),
            pltpu.VMEM((2 * CELLS_STEP * dates, dates), jnp.bfloat16),
            pltpu.VMEM((LINE_CELLS, 2, pairs), jnp.float32),
        ],
        compiler_params=pltpu.CompilerParams(
            dimension_semantics=("arbitrary",), vmem_limit_bytes=48 * 1024 * 1024
        ),
        name="cells",
    )(at, x, valid, table, second, first)


def line_blocks(samples):
    count, columns = samples.shape[:2]
    blocks = samples.reshape(count, columns, 2, BLOCKS, LANES).transpose(0, 1, 3, 2, 4)
    return blocks.reshape(count, columns * BLOCKS, 2, LANES)


def plane_terms(sums, along):
    w0, w1, w2, r0, r1, i0, i1 = (sums[k] for k in range(7))
    terms = (
        w0, w1, w0 * along, w2, w1 * along, w0 * along * along,
        r0, r1, r0 * along, i0, i1, i0 * along,
    )
    return jnp.stack(terms, 0)


def solve_three(n):
    adjugate_00 = n[3] * n[5] - n[4] * n[4]
    adjugate_01 = n[2] * n[4] - n[1] * n[5]
    adjugate_02 = n[1] * n[4] - n[2] * n[3]
    adjugate_11 = n[0] * n[5] - n[2] * n[2]
    adjugate_12 = n[1] * n[2] - n[0] * n[4]
    adjugate_22 = n[0] * n[3] - n[1] * n[1]
    determinant = n[0] * adjugate_00 + n[1] * adjugate_01 + n[2] * adjugate_02
    parts = []
    for t in (n[6:9], n[9:12]):
        parts.append(
            jnp.stack(
                [
                    adjugate_00 * t[0] + adjugate_01 * t[1] + adjugate_02 * t[2],
                    adjugate_01 * t[0] + adjugate_11 * t[1] + adjugate_12 * t[2],
                    adjugate_02 * t[0] + adjugate_12 * t[1] + adjugate_22 * t[2],
                ],
                0,
            )
            / determinant
        )
    return jnp.stack(parts, 0)


def summed_over(array, axis):
    copies = jnp.broadcast_to(array[None], (lax.axis_size(axis), *array.shape))
    return jnp.sum(lax.all_to_all(copies, axis, 0, 0, tiled=True), 0)


def along_of(position, range_cells):
    return (position.astype(jnp.float32) + 0.5) / range_cells - 0.5


def fitted(sums, range_cells):
    core = lax.axis_index("wide_2")
    position = lax.axis_index(WIDE)
    other = position + 1 - 2 * core
    swap = [(0, 1), (1, 0)]
    halves = sums.reshape(sums.shape[0], 2, -1)
    keep = jnp.where(core == 0, halves[:, 0], halves[:, 1])
    give = jnp.where(core == 0, halves[:, 1], halves[:, 0])
    got = lax.ppermute(give, "wide_2", swap)
    terms = plane_terms(keep, along_of(position, range_cells)) + plane_terms(
        got, along_of(other, range_cells)
    )
    ramps = solve_three(summed_over(summed_over(terms, "wide_1"), "wide_0"))
    others = lax.ppermute(ramps, "wide_2", swap)
    return jnp.where(
        core == 0, jnp.concatenate([ramps, others], -1), jnp.concatenate([others, ramps], -1)
    )


def local(slc, offsets, row_start, row_stop, pairs):
    devices = lax.axis_size(WIDE)
    position = lax.axis_index(WIDE)
    columns = slc.shape[1]
    here = columns // devices
    dates = devices * slc.shape[0]
    at = (LANES - here * (position % (LANES // here))) % LANES
    major, minor, cores = (lax.axis_size(axis) for axis in WIDE)
    samples = line_blocks(slc.reshape(devices, here, 2, AZ))
    sent = packed(samples.reshape(major, minor, cores, *samples.shape[1:]), offsets)
    received = lax.all_to_all(sent.reshape(devices, *sent.shape[3:]), SEND, 0, 0, tiled=True)
    lines = jnp.arange(AZ, dtype=jnp.int32)[None, :]
    valid = ((lines >= row_start[:, None]) & (lines < row_stop[:, None])).astype(jnp.float32)
    valid = valid.reshape(major, minor, cores, AZ).transpose(1, 2, 0, 3).reshape(dates, AZ)
    date = jnp.arange(dates, dtype=jnp.int32)[:, None]
    first = (date == pairs[:, 0][None, :]).astype(jnp.float32)
    second = (date == pairs[:, 1][None, :]).astype(jnp.bfloat16)
    coherence, ifg, sums = cells_call(
        major, cores, at.reshape(1), received.reshape(-1, LANES), valid, spectral_tables(), second, first
    )

    range_cells = columns // LOOK_RG
    ramps = fitted(sums, range_cells)
    share = pairs.shape[0] // devices
    own = lax.dynamic_slice_in_dim(ramps, position * share, share, 2).transpose(2, 0, 1)
    across = (jnp.arange(LINE_CELLS, dtype=jnp.int32).astype(jnp.float32) + 0.5) / LINE_CELLS - 0.5
    along = along_of(position, range_cells)
    plane = ramps[:, 0] + across[:, None, None] * ramps[:, 1] + along * ramps[:, 2]
    return coherence, ifg - plane, own


def solution(mesh):
    torus = Mesh(
        mesh.devices.reshape(mesh.shape["slab"], 8, 8, 2), ("slab", "wide_0", "wide_1", "wide_2")
    )
    in_specs = (P(WIDE, "slab", None, None), P(WIDE, "slab"), P(), P(), P())
    out_specs = (P(SLAB_WIDE, None, None, None), P(SLAB_WIDE, None, None), P(SLAB_WIDE, None, None))
    return jax.shard_map(local, mesh=torus, in_specs=in_specs, out_specs=out_specs, check_vma=False)
```
